128 devices in a mesh: pair: 8 (over x, core), aux: 16 (over y, z).
Axes of the slice: x: 4, y: 4, z: 4, core: 2. Of those that a mesh axis runs over, the one named last changes fastest.
Arguments:
- left_active: bfloat16 [80, 128, 61440], P('pair', None, 'aux'), may hold values from -0.375 to 0.375
- right_active: bfloat16 [80, 128, 61440], P('pair', None, 'aux'), may hold values from -0.375 to 0.375
- amps_active: bfloat16 [80, 128, 128], P('pair', 'aux'), may hold values from -0.5 to 0.5
- rank_active: int32 [80], P('pair'), may hold values from 80 to 128, as said below
- gap_active: float32 [80], P('pair'), may hold values from 0.5 to 2
- energy_active: float32 [80, 128], P('pair'), may hold values from 0.5 to 4
- intersect_active: bfloat16 [80, 4, 128, 128], P('pair'), may hold values from -0.75 to 0.75
- fock_active: float32 [80, 4], P('pair'), may hold values from -2 to 2
- neighbor_active: int32 [80, 4], P('pair'), may hold values from 0 to 79
- left_env: bfloat16 [32, 48, 61440], P('pair', None, 'aux'), may hold values from -0.375 to 0.375
- right_env: bfloat16 [32, 48, 61440], P('pair', None, 'aux'), may hold values from -0.375 to 0.375
- amps_env: bfloat16 [32, 48, 48], P('pair', 'aux'), may hold values from -0.875 to 0.875
- rank_env: int32 [32], P('pair'), may hold values from 24 to 48, as said below
- gap_env: float32 [32], P('pair'), may hold values from 0.5 to 2
- energy_env: float32 [32, 48], P('pair'), may hold values from 0.5 to 4
- intersect_env: bfloat16 [32, 4, 48, 48], P('pair'), may hold values from -1.25 to 1.25
- fock_env: float32 [32, 4], P('pair'), may hold values from -2 to 2
- neighbor_env: int32 [32, 4], P('pair'), may hold values from 0 to 31
Outputs:
- new_active: float32 [80, 128, 128], P('pair', 'aux')
- new_env: float32 [32, 48, 48], P('pair', 'aux')
The draws below stay inside these ranges and needn't reach their ends.
Inputs may be any that keep to these rules, and one draw needn't show every extreme that they name: `rank_active`: multiples of 8; the first active pair has rank 128. `rank_env`: multiples of 8; the first environment pair has rank 48.
All inputs are finite; a program needn't handle non-finite values.
Results may differ from the reference program's by a relative error of at most 0.0041.
Values may be sent and summed in bfloat16 or wider, within the bound.
A program may use at most 128 MiB of HBM per device.

```python
import math
import jax
import jax.numpy as jnp
from jax import lax

RA = 128
RE = 48
NAUX = 61440
NB = 4
PA = 80
PE = 32


def draw_rank_active(key, part):
    values = 8 * jax.random.randint(key, (PA,), RA * 5 // 64, RA // 8 + 1)
    return values.at[0].set(RA).astype(jnp.int32)


def draw_rank_env(key, part):
    values = 8 * jax.random.randint(key, (PE,), RE // 16, RE // 8 + 1)
    return values.at[0].set(RE).astype(jnp.int32)


def set_ends(array, key, least, high):
    longest = array.shape.index(max(array.shape))
    spots = []
    for shift in (0, 1):
        where = [jax.random.randint(jax.random.fold_in(key, axis), (), 0, length) for axis, length in enumerate(array.shape)]
        where[longest] = (where[longest] + shift) % array.shape[longest]
        spots.append(tuple(where))
    return array.at[spots[0]].set(least).at[spots[1]].set(high)


def block_scale(own_key, extent, shards, least, largest):
    factor_of = 1.0
    for position, blocks in shards:
        steps = jax.random.uniform(jax.random.fold_in(jax.random.fold_in(own_key, 6), position), (blocks,), jnp.float32, least / len(shards), largest / len(shards))
        factor_of = factor_of * jnp.repeat(jnp.exp(steps), extent[position] // blocks).reshape((-1,) + (1,) * (len(extent) - 1 - position))
    return factor_of


def normal_values(own_key, dims, width, most, pieces=(), held_as=jnp.bfloat16):
    factor_of = block_scale(own_key, dims, pieces, -0.22, 0.18) if pieces else 1.0
    entries = jax.random.normal(own_key, dims, jnp.float32) * width * factor_of
    return jnp.minimum(jnp.maximum(entries, -most), most).astype(held_as)


def setup_inputs(seed: int = 0) -> dict:
    key_list = jax.random.split(jax.random.key(seed), 19)
    left_active = normal_values(key_list[0], (PA, RA, NAUX), (NAUX ** -0.25), 0.375, ((0, 8), (2, 16)))
    right_active = normal_values(key_list[1], (PA, RA, NAUX), (NAUX ** -0.25), 0.375, ((0, 8), (2, 16)))
    amps_active = normal_values(key_list[2], (PA, RA, RA), (RA ** -0.5), 0.5, ((0, 8), (1, 16)))
    rank_active = draw_rank_active(jax.random.fold_in(key_list[18], 71), 0)
    gap_active = jnp.clip(jnp.exp(math.log(2.0) - 1.3862944 * jax.random.uniform(key_list[4], (PA,), jnp.float32) ** block_scale(key_list[4], (PA,), ((0, 8),), -0.2, 0.2)), 0.5, 2.0)
    energy_active = jnp.clip(jnp.exp(math.log(4.0) - 2.0794415 * jax.random.uniform(key_list[5], (PA, RA), jnp.float32) ** block_scale(key_list[5], (PA, RA), ((0, 8),), -0.2, 0.2)), 0.5, 4.0)
    intersect_active = normal_values(key_list[6], (PA, NB, RA, RA), (RA // 2) ** -0.5, 0.75, ((0, 8),))
    fock_active = jnp.clip(jax.random.uniform(key_list[7], (PA, NB), jnp.float32, -2.0, 2.0) * block_scale(key_list[7], (PA, NB), ((0, 8),), -0.4, 0.0), -2.0, 2.0)
    neighbor_active = set_ends(jax.random.randint(key_list[8], (PA, NB), 0, PA), jax.random.fold_in(key_list[8], 1), 0, PA - 1).astype(jnp.int32)
    left_env = normal_values(key_list[9], (PE, RE, NAUX), (NAUX ** -0.25), 0.375, ((0, 8), (2, 16)))
    right_env = normal_values(key_list[10], (PE, RE, NAUX), (NAUX ** -0.25), 0.375, ((0, 8), (2, 16)))
    amps_env = normal_values(key_list[11], (PE, RE, RE), (RE ** -0.5), 0.875, ((0, 8), (1, 16)))
    rank_env = draw_rank_env(jax.random.fold_in(key_list[18], 71), 0)
    gap_env = jnp.clip(jnp.exp(math.log(2.0) - 1.3862944 * jax.random.uniform(key_list[13], (PE,), jnp.float32) ** block_scale(key_list[13], (PE,), ((0, 8),), -0.2, 0.2)), 0.5, 2.0)
    energy_env = jnp.clip(jnp.exp(math.log(4.0) - 2.0794415 * jax.random.uniform(key_list[14], (PE, RE), jnp.float32) ** block_scale(key_list[14], (PE, RE), ((0, 8),), -0.2, 0.2)), 0.5, 4.0)
    intersect_env = normal_values(key_list[15], (PE, NB, RE, RE), (RE // 2) ** -0.5, 1.25, ((0, 8),))
    fock_env = jnp.clip(jax.random.uniform(key_list[16], (PE, NB), jnp.float32, -2.0, 2.0) * block_scale(key_list[16], (PE, NB), ((0, 8),), -0.4, 0.0), -2.0, 2.0)
    neighbor_env = set_ends(jax.random.randint(key_list[17], (PE, NB), 0, PE), jax.random.fold_in(key_list[17], 1), 0, PE - 1).astype(jnp.int32)
    return dict(left_active=left_active, right_active=right_active, amps_active=amps_active, rank_active=rank_active, gap_active=gap_active, energy_active=energy_active, intersect_active=intersect_active, fock_active=fock_active, neighbor_active=neighbor_active, left_env=left_env, right_env=right_env, amps_env=amps_env, rank_env=rank_env, gap_env=gap_env, energy_env=energy_env, intersect_env=intersect_env, fock_env=fock_env, neighbor_env=neighbor_env)


HIGHEST = lax.Precision.HIGHEST


def rank_masks(pair_ranks, full_width):
    positions = jnp.arange(full_width, dtype=jnp.int32)
    return (positions[None, :, None] < pair_ranks[:, None, None]) & (positions[None, None, :] < pair_ranks[:, None, None])


def update_level(left_ints, right_ints, amplitudes, pair_ranks, pair_gaps, energy, intersect, fock_weights, neighbor, with_ladder):
    full_width = amplitudes.shape[1]
    inside = rank_masks(pair_ranks, full_width)
    masked = jnp.where(inside, amplitudes, jnp.zeros_like(amplitudes))

    def one_pair(pair_items):
        left_pair, right_pair, amp_pair, over_pair, fock_pair, neigh_pair = pair_items
        summed_terms = jnp.dot(left_pair, right_pair.T, preferred_element_type=jnp.float32)
        if with_ladder:
            cross_left = jnp.dot(amp_pair.T, left_pair, preferred_element_type=jnp.float32).astype(jnp.bfloat16)
            cross_right = jnp.dot(amp_pair, right_pair, preferred_element_type=jnp.float32).astype(jnp.bfloat16)
            summed_terms = summed_terms + jnp.dot(cross_left, right_pair.T, preferred_element_type=jnp.float32)
            summed_terms = summed_terms + jnp.dot(cross_left, cross_right.T, preferred_element_type=jnp.float32)
        near_amps = masked[neigh_pair]
        half_product = jnp.einsum('krs,kst->krt', over_pair, near_amps, preferred_element_type=jnp.float32)
        full_product = jnp.einsum('krt,kut->kru', half_product, over_pair.astype(jnp.float32), precision=HIGHEST)
        return summed_terms + jnp.einsum('k,kru->ru', fock_pair, full_product, precision=HIGHEST)

    residual = lax.map(one_pair, (left_ints, right_ints, masked, intersect, fock_weights, neighbor))
    denominator = energy[:, :, None] + energy[:, None, :] + pair_gaps[:, None, None]
    return jnp.where(inside, masked.astype(jnp.float32) - residual / denominator, jnp.float32(0.0))


def reference(left_active, right_active, amps_active, rank_active, gap_active, energy_active, intersect_active, fock_active, neighbor_active, left_env, right_env, amps_env, rank_env, gap_env, energy_env, intersect_env, fock_env, neighbor_env):
    new_active = update_level(left_active, right_active, amps_active, rank_active, gap_active, energy_active, intersect_active, fock_active, neighbor_active, True)
    new_env = update_level(left_env, right_env, amps_env, rank_env, gap_env, energy_env, intersect_env, fock_env, neighbor_env, False)
    return (new_active, new_env)
```

```python
import functools

import jax
import jax.numpy as jnp
from jax import lax
from jax.experimental import pallas as pl
from jax.experimental.pallas import tpu as pltpu
from jax.sharding import PartitionSpec as P

MESH = pl.DeviceIdType.MESH
F32 = jnp.float32
BF16 = jnp.bfloat16
NT = (((1,), (1,)), ((), ()))
TN = (((0,), (0,)), ((), ()))
AHEAD = 3


def iota(shape, dim):
    return lax.broadcasted_iota(jnp.int32, shape, dim)


def nt(a, b):
    return lax.dot_general(a, b, NT, preferred_element_type=F32)


def mm(a, b):
    return jnp.dot(a, b, preferred_element_type=F32)


def kernel(
    n_aux,
    n_pair,
    rank_a,
    gap_a,
    fock_a,
    near_a,
    rank_e,
    gap_e,
    fock_e,
    near_e,
    amps_a,
    amps_e,
    energy_a,
    energy_e,
    left_a,
    right_a,
    over_a,
    left_e,
    right_e,
    over_e,
    out_a,
    out_e,
    lbuf,
    rbuf,
    lebuf,
    rebuf,
    obuf,
    oebuf,
    wbuf,
    webuf,
    own_a,
    own_e,
    tall,
    near_rows_a,
    near_rows_e,
    part,
    got,
    l_sem,
    r_sem,
    le_sem,
    re_sem,
    o_sem,
    tsend,
    trecv,
    pasend,
    parecv,
    pesend,
    perecv,
    ssend,
    srecv,
):
    pairs = left_a.shape[0]
    envs = left_e.shape[0]
    nb = over_a.shape[1]
    re_ = left_e.shape[1]
    rows_e = amps_e.shape[0]
    me = lax.axis_index("pair")
    j = lax.axis_index("aux")

    def load_pair(p):
        return (
            pltpu.make_async_copy(left_a.at[p], lbuf.at[p], l_sem.at[p]),
            pltpu.make_async_copy(right_a.at[p], rbuf.at[p], r_sem.at[p]),
        )

    def start_pair(p):
        for copy in load_pair(p):
            copy.start()

    def load_env(q):
        c, i = q // 2, q % 2
        return (
            pltpu.make_async_copy(left_e.at[q], lebuf.at[c, pl.ds(i * re_, re_)], le_sem.at[q]),
            pltpu.make_async_copy(right_e.at[q], rebuf.at[c, pl.ds(i * 64, re_)], re_sem.at[q]),
        )

    over_copies = (
        pltpu.make_async_copy(over_a, obuf, o_sem.at[0]),
        pltpu.make_async_copy(over_e, oebuf, o_sem.at[1]),
    )
    for p in range(AHEAD):
        start_pair(p)
    for copy in over_copies:
        copy.start()

    barrier = pltpu.get_barrier_semaphore()

    @pl.loop(1, n_aux)
    def _(o):
        pl.semaphore_signal(barrier, inc=1, device_id={"aux": lax.rem(j + o, n_aux)}, device_id_type=MESH)

    @pl.loop(1, n_pair)
    def _(o):
        pl.semaphore_signal(barrier, inc=1, device_id={"pair": lax.rem(me + o, n_pair)}, device_id_type=MESH)

    lanes8 = iota((8, 128), 1)
    subs8 = iota((8, 128), 0)
    for p in range(pairs):
        rank = rank_a[p]
        inside = (subs8 + 8 * j < rank) & (lanes8 < rank)
        own_a[p] = jnp.where(inside, amps_a[p].astype(F32), 0.0).astype(BF16)
    for q in range(envs):
        rank = rank_e[q]
        slab = jnp.zeros((8, 128), F32)
        for r in range(rows_e):
            line = jnp.pad(amps_e[r].astype(F32)[q : q + 1], ((0, 0), (0, 128 - re_)))
            slab = jnp.where(subs8 == r, line, slab)
        inside = (subs8 + rows_e * j < rank) & (lanes8 < rank) & (subs8 < rows_e)
        own_e[q] = jnp.where(inside, slab, 0.0).astype(BF16)
    tall[j] = own_a[...]
    near_rows_a[pl.ds(me * pairs, pairs)] = own_a[...]
    near_rows_e[pl.ds(me * envs, envs)] = own_e[...]

    pl.semaphore_wait(barrier, n_aux - 1 + n_pair - 1)

    def send_t(o):
        return pltpu.make_async_remote_copy(
            own_a, tall.at[j], tsend.at[o], trecv.at[o],
            device_id={"aux": lax.rem(j + o, n_aux)}, device_id_type=MESH,
        )

    def send_pa(o):
        return pltpu.make_async_remote_copy(
            own_a, near_rows_a.at[pl.ds(me * pairs, pairs)], pasend.at[o], parecv.at[o],
            device_id={"pair": lax.rem(me + o, n_pair)}, device_id_type=MESH,
        )

    def send_pe(o):
        return pltpu.make_async_remote_copy(
            own_e, near_rows_e.at[pl.ds(me * envs, envs)], pesend.at[o], perecv.at[o],
            device_id={"pair": lax.rem(me + o, n_pair)}, device_id_type=MESH,
        )

    @pl.loop(1, n_aux)
    def _(o):
        send_t(o).start()

    @pl.loop(1, n_pair)
    def _(o):
        send_pa(o).start()
        send_pe(o).start()

    @pl.loop(0, pairs // 2)
    def _(h):
        for i in range(2):
            p = 2 * h + i

            @pl.when(p + AHEAD < pairs)
            def _():
                start_pair(p + AHEAD)

            if i == 1:

                @pl.when(h == pairs // 2 - 2)
                def _():
                    for q in range(envs):
                        for copy in load_env(q):
                            copy.start()

        for i in range(2):
            for copy in load_pair(2 * h + i):
                copy.wait()
        for i in range(2):
            wbuf[2 * h + i] = nt(lbuf[2 * h + i], rbuf[2 * h + i])

    lanes48 = iota((re_, 128), 1)
    for q in range(envs):
        for copy in load_env(q):
            copy.wait()
    for c in range(envs // 2):
        both = nt(lebuf[c], rebuf[c])
        webuf[c] = jnp.where(lanes48 < 64, both[:re_], both[re_:])

    for copy in over_copies:
        copy.wait()

    @pl.loop(1, n_pair)
    def _(o):
        send_pa(o).wait()
        send_pe(o).wait()

    @pl.loop(1, n_aux)
    def _(o):
        send_t(o).wait()

    pick_a = (lanes8 == subs8 + 8 * j).astype(F32)
    pick_e = ((lanes8 == subs8 + rows_e * j) & (subs8 < rows_e)).astype(F32)
    blank = jnp.zeros((8, 128), F32)

    def coupling(over, rows, pick, focks):
        total = None
        for k in range(nb):
            blocks = [blank] * 16
            blocks[k] = rows[k]
            blocks[4 + k] = rows[k]
            blocks[8 + k] = pick
            blocks[12 + k] = pick
            side = jnp.concatenate(blocks, axis=0).astype(BF16)
            term = nt(over[k], side[:, : over[k].shape[1]])
            total = term if total is None else total + term
        lane = iota(total.shape, 1)
        weight = jnp.zeros(total.shape, F32)
        for k in range(nb):
            weight = jnp.where((lane // 8) % 4 == k, focks[k], weight)
        scaled = total * weight
        high = scaled.astype(BF16).astype(F32)
        split = jnp.where(lane < 32, high, jnp.where(lane < 64, scaled - high, 0.0)).astype(BF16)
        cols = pltpu.roll(total, 64, 1).astype(BF16)
        return cols, split

    @pl.loop(0, pairs // 2)
    def _(h):
        for i in range(2):
            p = 2 * h + i
            t = tall[:, p].astype(F32).reshape(128, 128).astype(BF16)
            w = wbuf[p]
            v = lax.dot_general(t, w.astype(BF16), TN, preferred_element_type=F32)
            x = nt(v.astype(BF16), t)
            rows = [near_rows_a[near_a[k, p]].astype(F32) for k in range(nb)]
            cols, split = coupling([obuf[p, k] for k in range(nb)], rows, pick_a, [fock_a[k, p] for k in range(nb)])
            whole = w + v + x + nt(cols, split)
            part[:, p] = whole.reshape(n_aux, 8, 128).astype(BF16)

    place = iota((128, re_), 0)
    line = iota((128, re_), 1)
    packed = None
    for c in range(envs // 2):
        pieces = []
        sides = []
        for i in range(2):
            q = 2 * c + i
            rows = [near_rows_e[near_e[q, k]].astype(F32) for k in range(nb)]
            cols, split = coupling([oebuf[q, k] for k in range(nb)], rows, pick_e, [fock_e[q, k] for k in range(nb)])
            pieces.append(cols)
            sides.append(split.astype(F32))
        gap = jnp.zeros((64 - re_, 128), F32)
        side = jnp.concatenate([sides[0], gap, sides[1], gap], axis=0).astype(BF16)
        couple = jnp.where(lanes48 < 64, nt(pieces[0], side), nt(pieces[1], side))
        whole = jnp.where((lanes48 % 64) < re_, webuf[c] + couple, 0.0).astype(BF16)
        perm = (place % 8 >= rows_e * c) & (place % 8 < rows_e * (c + 1)) & (
            line == rows_e * (place // 8) + place % 8 - rows_e * c
        )
        moved = mm(perm.astype(F32).astype(BF16), whole)
        packed = moved if packed is None else packed + moved
    part[:, pairs] = packed.reshape(n_aux, 8, 128).astype(BF16)

    def send_s(o):
        d = lax.rem(j + o, n_aux)
        return pltpu.make_async_remote_copy(
            part.at[d], got.at[j], ssend.at[o], srecv.at[o],
            device_id={"aux": d}, device_id_type=MESH,
        )

    @pl.loop(1, n_aux)
    def _(o):
        send_s(o).start()

    got[j] = part[j]

    @pl.loop(1, n_aux)
    def _(o):
        send_s(o).wait()

    for p in range(pairs):
        total = got[0, p].astype(F32)
        for d in range(1, n_aux):
            total = total + got[d, p].astype(F32)
        rank = rank_a[p]
        inside = (subs8 + 8 * j < rank) & (lanes8 < rank)
        across = energy_a[pl.ds(p, 1), :]
        down = jnp.sum(jnp.where(lanes8 == subs8 + 8 * j, across, 0.0), axis=1, keepdims=True)
        out_a[p] = jnp.where(inside, own_a[p].astype(F32) - total / (down + across + gap_a[p]), 0.0)

    total = got[0, pairs].astype(F32)
    for d in range(1, n_aux):
        total = total + got[d, pairs].astype(F32)
    for q in range(envs):
        c, i = q // 2, q % 2
        mine = pltpu.roll(total, 64, 1) if i else total
        if c:
            mine = pltpu.roll(mine, 8 - rows_e, 0)
        rank = rank_e[q]
        inside = (subs8 + rows_e * j < rank) & (lanes8 < rank) & (subs8 < rows_e)
        across = jnp.pad(energy_e[pl.ds(q, 1), :], ((0, 0), (0, 128 - re_)))
        down = jnp.sum(jnp.where(lanes8 == subs8 + rows_e * j, across, 0.0), axis=1, keepdims=True)
        new = jnp.where(inside, own_e[q].astype(F32) - mine / (down + across + gap_e[q]), 0.0)
        for r in range(rows_e):
            out_e[r, pl.ds(q, 1), :] = new[r : r + 1, :re_]


def shards(
    left_a, right_a, amps_a, rank_a, gap_a, energy_a, over_a, fock_a, near_a,
    left_e, right_e, amps_e, rank_e, gap_e, energy_e, over_e, fock_e, near_e,
):
    n_aux, n_pair = 16, 8
    pairs, full, depth = left_a.shape
    envs, re_, _ = left_e.shape
    rows_e = amps_e.shape[1]
    nb = over_a.shape[1]
    smem = pl.BlockSpec(memory_space=pltpu.SMEM)
    vmem = pl.BlockSpec(memory_space=pltpu.VMEM)
    hbm = pl.BlockSpec(memory_space=pltpu.HBM)
    dma = pltpu.SemaphoreType.DMA
    slots = pairs + 1
    new_a, new_e = pl.pallas_call(
        functools.partial(kernel, n_aux, n_pair),
        out_shape=(
            jax.ShapeDtypeStruct((pairs, 8, full), F32),
            jax.ShapeDtypeStruct((rows_e, envs, re_), F32),
        ),
        in_specs=[smem] * 8 + [vmem] * 4 + [hbm] * 6,
        out_specs=(vmem, vmem),
        scratch_shapes=[
            pltpu.VMEM((pairs, full, depth), BF16),
            pltpu.VMEM((pairs, full, depth), BF16),
            pltpu.VMEM((envs // 2, 2 * re_, depth), BF16),
            pltpu.VMEM((envs // 2, 128, depth), BF16),
            pltpu.VMEM((pairs, nb, full, full), BF16),
            pltpu.VMEM((envs, nb, re_, re_), BF16),
            pltpu.VMEM((pairs, full, full), F32),
            pltpu.VMEM((envs // 2, re_, 128), F32),
            pltpu.VMEM((pairs, 8, 128), BF16),
            pltpu.VMEM((envs, 8, 128), BF16),
            pltpu.VMEM((n_aux, pairs, 8, 128), BF16),
            pltpu.VMEM((n_pair * pairs, 8, 128), BF16),
            pltpu.VMEM((n_pair * envs, 8, 128), BF16),
            pltpu.VMEM((n_aux, slots, 8, 128), BF16),
            pltpu.VMEM((n_aux, slots, 8, 128), BF16),
            dma((pairs,)),
            dma((pairs,)),
            dma((envs,)),
            dma((envs,)),
            dma((2,)),
            dma((n_aux,)),
            dma((n_aux,)),
            dma((n_pair,)),
            dma((n_pair,)),
            dma((n_pair,)),
            dma((n_pair,)),
            dma((n_aux,)),
            dma((n_aux,)),
        ],
        compiler_params=pltpu.CompilerParams(
            collective_id=0, has_side_effects=True, vmem_limit_bytes=56 * 2**20
        ),
        name="update",
    )(
        rank_a, gap_a, fock_a.T, near_a.T, rank_e, gap_e, fock_e, near_e,
        amps_a, jnp.swapaxes(amps_e, 0, 1), energy_a, energy_e,
        left_a, right_a, over_a, left_e, right_e, over_e,
    )
    return new_a, jnp.swapaxes(new_e, 0, 1)


def solution(mesh):
    p = P
    return jax.shard_map(
        shards,
        mesh=mesh,
        in_specs=(
            p("pair", None, "aux"), p("pair", None, "aux"), p("pair", "aux", None), p("pair"), p("pair"),
            p("pair", None), p("pair", None, None, None), p("pair", None), p("pair", None),
            p("pair", None, "aux"), p("pair", None, "aux"), p("pair", "aux", None), p("pair"), p("pair"),
            p("pair", None), p("pair", None, None, None), p("pair", None), p("pair", None),
        ),
        out_specs=(p("pair", "aux", None), p("pair", "aux", None)),
        check_vma=False,
    )
```
